32 devices in a mesh: lat: 16 (over z, y, x), ord: 2 (over core).
Axes of the slice: x: 2, y: 2, z: 4, core: 2. Of those that a mesh axis runs over, the one named last changes fastest.
Arguments:
- pressure: bfloat16 [2, 128, 5760], P(None, 'lat', 'ord'), may hold values from -6 to 6
- tables: bfloat16 [512, 128, 2048], P('ord', 'lat'), may hold values from -6 to 6
- quad_weight: float32 [128], replicated, may hold values from 0.5 to 2
- love_number: float32 [2048], replicated, may hold values from -0.5 to 0
- order_list: int32 [512], replicated, may hold values from 0 to 511, each once
- cycle_list: int32 [128], P('lat'), may hold values from 0 to 127, each once
Outputs:
- spectrum: float32 [2, 512, 2048], P(None, 'ord', 'lat')
- load_field: float32 [2, 128, 5760], P(None, 'lat', 'ord')
The draws below stay inside these ranges and needn't reach their ends.
Inputs may be any that keep to these rules, and one draw needn't show every extreme that they name: `order_list`: every order from 0 to 511 stands in exactly one slot. `cycle_list`: every northern cycle from 0 to 127 stands in exactly one slot; the same slot of the southern half holds its mirror cycle.
All inputs are finite; a program needn't handle non-finite values.
Results may differ from the reference program's by a relative error of at most 0.0055.
Values may be sent and summed in bfloat16 or wider, within the bound.
A program may use at most 64 MiB of HBM per device.

```python
import math
import jax
import jax.numpy as jnp
from jax import lax

NLON = 5760
LDEG = 2048
NORD = 512
NHALF = 128


def with_spikes(array, stream_key, source, target, blocks, factor):
    def block_of(dim):
        return (jnp.arange(array.shape[dim]) // (array.shape[dim] // blocks)).reshape((-1,) + (1,) * (array.ndim - 1 - dim))

    near = jax.random.permutation(stream_key, blocks)[block_of(target)]
    other_side = (block_of(target) + blocks // 2) % blocks
    return jnp.where((block_of(source) == near) | (block_of(source) == other_side), factor * array, array)


def levels(stream_key, extent, pieces, smallest, high):
    level, own = 1.0, jax.random.fold_in(stream_key, 6)
    for dim, blocks in pieces:
        draws = jnp.exp(jax.random.uniform(jax.random.fold_in(own, dim), (blocks,), jnp.float32, smallest / len(pieces), high / len(pieces)))
        level = level * jnp.repeat(draws, extent[dim] // blocks).reshape([-1 if axis == dim else 1 for axis in range(len(extent))])
    return level


def normal_values(own_key, dims, scale, limit, cuts=(), kind=jnp.bfloat16):
    result = jax.random.normal(own_key, dims, jnp.float32) * scale
    if len(cuts) > 0:
        result = levels(own_key, dims, cuts, -0.22, 0.18) * result
    return jnp.clip(result, min=-limit, max=limit).astype(kind)


def heavy_noise(own_key, extent, scale, reach, pieces, heavy, held_as=jnp.bfloat16):
    values = scale * jax.random.normal(own_key, extent, jnp.float32)
    if pieces:
        values = values * levels(own_key, extent, pieces, -0.22, 0.18)
    return jnp.clip(with_spikes(values, jax.random.fold_in(own_key, 3), *heavy), -reach, reach).astype(held_as)


def setup_inputs(seed: int = 0) -> dict:
    splits = jax.random.split(jax.random.key(seed), 7)
    return {
        "pressure": normal_values(splits[0], (2, NHALF, NLON), 1.0, 6.0, ((1, 16), (2, 2))),
        "tables": heavy_noise(splits[1], (NORD, NHALF, LDEG), 1.0, 6.0, ((0, 2), (1, 16)), (1, 2, 16, 2.0)),
        "quad_weight": jnp.clip(jnp.exp(jax.random.uniform(splits[2], (NHALF,), jnp.float32, math.log(0.5), math.log(2.0))), 0.5, 2.0),
        "love_number": jnp.clip(jax.random.uniform(splits[3], (LDEG,), jnp.float32, -0.5, 0.0), -0.5, 0.0),
        "order_list": jax.random.permutation(splits[4], NORD).astype(jnp.int32),
        "cycle_list": jax.random.permutation(splits[5], NHALF).astype(jnp.int32),
    }


DENSITY_RATIO = 3.0 * 1025.0 / 5517.0

def phase_table(order_values, positions):
    phase = order_values[:, None] * positions[None, :] % NLON
    angle = phase.astype(jnp.float32) * (2.0 * math.pi / NLON)
    return (jnp.cos(angle).astype(jnp.bfloat16), jnp.sin(angle).astype(jnp.bfloat16))

def reference(pressure, tables, quad_weight, love_number, order_list, cycle_list):
    grid_rows = pressure.reshape(2 * NHALF, NLON)
    cosine_table, sine_table = phase_table(order_list, jnp.arange(NLON, dtype=jnp.int32))
    lon_scale = 1.0 / math.sqrt(NLON)
    real_part = lon_scale * jnp.dot(grid_rows, cosine_table.T, preferred_element_type=jnp.float32)
    imag_part = -lon_scale * jnp.dot(grid_rows, sine_table.T, preferred_element_type=jnp.float32)
    cycle_weight = (quad_weight[cycle_list] * (1.0 / math.sqrt(NHALF)))[:, None]
    north_real = real_part[:NHALF]
    south_real = real_part[NHALF:]
    north_imag = imag_part[:NHALF]
    south_imag = imag_part[NHALF:]
    folded = jnp.stack([cycle_weight * (north_real + south_real), cycle_weight * (north_imag + south_imag), cycle_weight * (north_real - south_real), cycle_weight * (north_imag - south_imag)], 0)
    folded = jnp.transpose(folded.astype(jnp.bfloat16), (2, 1, 0))
    degree = jnp.arange(LDEG, dtype=jnp.int32)

    def analyse(item):
        table, column, order_value = item
        product = jnp.dot(column.T, table, preferred_element_type=jnp.float32)
        even = (degree + order_value) % 2 == 0
        present = degree >= order_value
        coeff_real = jnp.where(present, jnp.where(even, product[0], product[2]), 0.0)
        coeff_imag = jnp.where(present, jnp.where(even, product[1], product[3]), 0.0)
        return jnp.stack([coeff_real, coeff_imag], 0)
    coefficients = lax.map(analyse, (tables, folded, order_list))
    spectrum = jnp.transpose(coefficients, (1, 0, 2))
    love_factor = DENSITY_RATIO * (1.0 + love_number)
    scaled = (love_factor * coefficients).astype(jnp.bfloat16)
    deg_scale = 1.0 / math.sqrt(LDEG)

    def synthesise(item):
        table, coeff, order_value = item
        even = (degree + order_value) % 2 == 0
        zero = jnp.zeros_like(coeff[0])
        stacked = jnp.stack([jnp.where(even, coeff[0], zero), jnp.where(even, coeff[1], zero), jnp.where(even, zero, coeff[0]), jnp.where(even, zero, coeff[1])], 0)
        summed = jnp.dot(table, stacked.T, preferred_element_type=jnp.float32)
        north = deg_scale * (summed[:, :2] + summed[:, 2:])
        south = deg_scale * (summed[:, :2] - summed[:, 2:])
        return jnp.stack([north, south], 0).astype(jnp.bfloat16)
    synthesised = lax.map(synthesise, (tables, scaled, order_list))
    synth_real = synthesised[..., 0].reshape(NORD, 2 * NHALF)
    synth_imag = synthesised[..., 1].reshape(NORD, 2 * NHALF)
    field = jnp.dot(synth_real.T, cosine_table, preferred_element_type=jnp.float32) - jnp.dot(synth_imag.T, sine_table, preferred_element_type=jnp.float32)
    load_field = (1.0 / math.sqrt(NORD) * field).reshape(2, NHALF, NLON)
    return (spectrum, load_field)
```

```python
import functools
import math

import jax
import jax.numpy as jnp
from jax import lax
from jax.experimental import pallas as pl
from jax.experimental.pallas import tpu as pltpu
from jax.sharding import PartitionSpec as P

DENSITY_RATIO = 3.0 * 1025.0 / 5517.0
LANES = 128
GROUPS = 8
STAGGER = 2
MESH = pl.DeviceIdType.MESH
NT = (((1,), (1,)), ((), ()))
F32 = jnp.float32
BF16 = jnp.bfloat16


def bit_orders(bits):
    base = list(range(bits))
    if bits < 3:
        return [base] * GROUPS
    a = base
    b = [1, 0] + base[2:]
    c = [2, 0, 1] + base[3:]
    d = [2, 1, 0] + base[3:]
    return [a, b, c, a, b, d, a, b]


def permuted(index, order):
    bits = len(order)
    return sum(((index // 2**b) % 2) * 2 ** (bits - 1 - at) for at, b in enumerate(order))


def kernel(
    n, no, cycles, half_lon,
    press_ref, tables_ref, cos_q, sin_q, cos_r, sin_r, orders_ref, fold_ref, sel_ref, love_ref,
    spec_ref, field_ref,
    tab, wave, gathered, lhs, part, landed, scaled, picked, out_piece, in_piece,
    tab_sem, press_sem, rs_sem, ag_sem, field_sem,
):
    bits = n.bit_length() - 1
    me = lax.axis_index("lat")
    core = lax.axis_index("ord")
    local_orders = orders_ref.shape[0]
    degrees = tables_ref.shape[1]
    share = degrees // n
    go = local_orders // GROUPS
    rows_g = go * cycles
    blocks = max(1, min(n, 1024 // share))
    width = blocks * share
    orders_of = bit_orders(bits)
    lon_pad = wave.shape[3]

    barrier = pltpu.get_barrier_semaphore()
    partners = []
    for b in range(bits):
        mine = (me // 2**b) % 2
        partners.append(me + (1 - 2 * mine) * 2**b)
    peers = [lax.rem(core + i, no) for i in range(1, no)]
    for partner in partners:
        pl.semaphore_signal(barrier, inc=1, device_id=(partner, core), device_id_type=MESH)
    for peer in peers:
        pl.semaphore_signal(barrier, inc=1, device_id=(me, peer), device_id_type=MESH)

    tab_copies = []
    for g in range(GROUPS):
        rows = pl.ds(g * rows_g, rows_g)
        copy = pltpu.make_async_copy(tables_ref.at[rows], tab.at[rows], tab_sem.at[g])
        copy.start()
        tab_copies.append(copy)

    pl.semaphore_wait(barrier, bits + no - 1)
    press_copies = []
    for i, peer in enumerate(peers):
        copy = pltpu.make_async_remote_copy(
            src_ref=press_ref,
            dst_ref=gathered.at[i],
            send_sem=press_sem.at[0, i],
            recv_sem=press_sem.at[1, i],
            device_id=(me, peer),
            device_id_type=MESH,
        )
        copy.start()
        press_copies.append(copy)

    def make_wave(p, carry):
        for q in range(lon_pad // LANES):
            cq = cos_q[p, :, q : q + 1]
            sq = sin_q[p, :, q : q + 1]
            cols = slice(q * LANES, (q + 1) * LANES)
            wave[p, 0, :, cols] = (cq * cos_r[...] - sq * sin_r[...]).astype(BF16)
            wave[p, 1, :, cols] = (sq * cos_r[...] + cq * sin_r[...]).astype(BF16)
        return carry

    lax.fori_loop(0, no, make_wave, 0)

    sums = [jnp.zeros((local_orders, press_ref.shape[0]), F32) for _ in range(2)]
    for i in range(no):
        if i > 0:
            press_copies[i - 1].wait()
        origin = lax.rem(core + no - i, no)
        rows = press_ref[...] if i == 0 else gathered[i - 1]
        for t in range(2):
            sums[t] = sums[t] + lax.dot_general(wave[origin, t], rows, NT, preferred_element_type=F32)

    col = lax.broadcasted_iota(jnp.int32, (local_orders, rows_g), 1) // cycles
    row = lax.broadcasted_iota(jnp.int32, (local_orders, rows_g), 0) % go
    diagonal = row == col
    for f in range(2):
        for t in range(2):
            value = lax.dot_general(
                sums[t], fold_ref[2 * f + t], (((1,), (0,)), ((), ())),
                precision=lax.Precision.HIGHEST, preferred_element_type=F32,
            )
            lhs[2 * f + t] = jnp.where(diagonal, value, 0.0)

    def parity(g, first):
        degree = first + lax.broadcasted_iota(jnp.int32, (go, width), 1)
        order = orders_ref[g * go : (g + 1) * go, :]
        return (degree + order) & 1 == 0, degree >= order

    def region(g, k):
        base = 0
        for at in range(k):
            base = base + ((me // 2 ** orders_of[g][at]) % 2) * (n >> (at + 1))
        return base

    def analyse(g):
        tab_copies[g].wait()
        left = jnp.concatenate([lhs[c, g * go : (g + 1) * go, :] for c in range(4)], 0).astype(BF16)

        def chunk(i, carry):
            first = pl.multiple_of(i * width, width)
            product = jnp.dot(
                left, tab[g * rows_g : (g + 1) * rows_g, pl.ds(first, width)], preferred_element_type=F32
            )
            even, present = parity(g, first)
            real = jnp.where(present, jnp.where(even, product[:go], product[2 * go : 3 * go]), 0.0)
            imag = jnp.where(present, jnp.where(even, product[go : 2 * go], product[3 * go :]), 0.0)
            value = jnp.concatenate([real, imag], 0).astype(BF16)
            for j in range(blocks):
                to = permuted(i * blocks + j, orders_of[g])
                part[g, to] = value[:, j * share : (j + 1) * share]
            return carry

        lax.fori_loop(0, degrees // width, chunk, 0)

    reduce_copies = {}
    gather_copies = {}

    def send_reduce(g, k):
        h = n >> (k + 1)
        b = orders_of[g][k]
        mine = (me // 2**b) % 2
        copy = pltpu.make_async_remote_copy(
            src_ref=part.at[g, pl.ds(region(g, k) + (1 - mine) * h, h)],
            dst_ref=landed.at[g, pl.ds(n - (n >> k), h)],
            send_sem=rs_sem.at[0, g, k],
            recv_sem=rs_sem.at[1, g, k],
            device_id=(partners[b], core),
            device_id_type=MESH,
        )
        copy.start()
        reduce_copies[g, k] = copy

    def take_reduce(g, k):
        h = n >> (k + 1)
        reduce_copies[g, k].wait_recv()
        keep = region(g, k + 1)
        off = n - (n >> k)
        if k < bits - 1:

            def add(i, carry):
                part[g, keep + i] = (
                    part[g, keep + i].astype(F32) + landed[g, off + i].astype(F32)
                ).astype(BF16)
                return carry

            lax.fori_loop(0, h, add, 0, unroll=min(h, 4))
            send_reduce(g, k + 1)
            return
        total = part[g, keep].astype(F32) + landed[g, off].astype(F32)
        spec_ref[0, g * go : (g + 1) * go, :] = total[:go]
        spec_ref[1, g * go : (g + 1) * go, :] = total[go:]
        scaled[g, keep] = (love_ref[...] * total).astype(BF16)
        send_gather(g, bits - 1)

    def send_gather(g, k):
        h = n >> (k + 1)
        b = orders_of[g][k]
        mine = pl.ds(region(g, k + 1), h)
        copy = pltpu.make_async_remote_copy(
            src_ref=scaled.at[g, mine],
            dst_ref=scaled.at[g, mine],
            send_sem=ag_sem.at[0, g, k],
            recv_sem=ag_sem.at[1, g, k],
            device_id=(partners[b], core),
            device_id_type=MESH,
        )
        copy.start()
        gather_copies[g, k] = copy

    def take_gather(g, k):
        gather_copies[g, k].wait_recv()
        if k > 0:
            send_gather(g, k - 1)

    def synthesise(g):
        def chunk(i, total):
            first = pl.multiple_of(i * width, width)
            even, _ = parity(g, first)
            pieces = [scaled[g, permuted(i * blocks + j, orders_of[g])] for j in range(blocks)]
            both = jnp.concatenate(pieces, 1).astype(F32)
            real, imag = both[:go], both[go:]
            stacked = jnp.concatenate(
                [real, imag, jnp.where(even, real, -real), jnp.where(even, imag, -imag)], 0
            ).astype(BF16)
            return total + lax.dot_general(
                stacked, tab[g * rows_g : (g + 1) * rows_g, pl.ds(first, width)], NT,
                preferred_element_type=F32,
            )

        total = lax.fori_loop(0, degrees // width, chunk, jnp.zeros((4 * go, rows_g), F32))
        total = total * (1.0 / math.sqrt(degrees))
        keep = diagonal[:go]
        for c in range(4):
            picked[c, g * go : (g + 1) * go, :] = jnp.where(keep, total[c * go : (c + 1) * go], 0.0)

    steps = []
    for g in range(GROUPS):
        steps.append((g, g, lambda g=g: (analyse(g), send_reduce(g, 0))))
        for k in range(bits):
            steps.append((g + STAGGER * (k + 1), g, lambda g=g, k=k: take_reduce(g, k)))
        for i, k in enumerate(reversed(range(bits))):
            steps.append((g + STAGGER * (bits + i + 1), g, lambda g=g, k=k: take_gather(g, k)))
        steps.append((g + STAGGER * 2 * bits + 1, g, lambda g=g: synthesise(g)))
    for _, _, step in sorted(steps, key=lambda s: (s[0], s[1])):
        step()

    signal = []
    for t in range(2):
        north = lax.dot_general(sel_ref[0], picked[t].astype(BF16), NT, preferred_element_type=F32)
        south = lax.dot_general(sel_ref[1], picked[2 + t].astype(BF16), NT, preferred_element_type=F32)
        signal.append((north + south).astype(BF16))
    signal[1] = -signal[1]

    def piece(p):
        total = jnp.dot(signal[0], wave[p, 0], preferred_element_type=F32)
        return total + jnp.dot(signal[1], wave[p, 1], preferred_element_type=F32)

    field_copies = []
    for i, peer in enumerate(peers):
        out_piece[i] = piece(peer)
        copy = pltpu.make_async_remote_copy(
            src_ref=out_piece.at[i],
            dst_ref=in_piece.at[i],
            send_sem=field_sem.at[0, i],
            recv_sem=field_sem.at[1, i],
            device_id=(me, peer),
            device_id_type=MESH,
        )
        copy.start()
        field_copies.append(copy)
    total = piece(core)
    for i, copy in enumerate(field_copies):
        copy.wait_recv()
        total = total + in_piece[i]
    field_ref[...] = total[:, :half_lon] * (1.0 / math.sqrt(local_orders * no))
    for copy in list(reduce_copies.values()) + list(gather_copies.values()) + field_copies:
        copy.wait_send()


def cos_sin(phase, period):
    angle = (phase % period).astype(F32) * (2.0 * math.pi / period)
    return jnp.cos(angle), jnp.sin(angle)


def per_device(n, no, pressure, tables, quad_weight, love_number, order_list, cycle_list):
    cycles = pressure.shape[1]
    lon_local = pressure.shape[2]
    local_orders = tables.shape[0]
    degrees = tables.shape[2]
    half_total = quad_weight.shape[0]
    period = lon_local * no
    bits = n.bit_length() - 1
    share = degrees // n
    go = local_orders // GROUPS
    rows_g = go * cycles
    tiles = -(-lon_local // LANES)
    lon_pad = tiles * LANES
    my_orders = lax.dynamic_slice_in_dim(
        order_list, lax.axis_index("ord") * local_orders, local_orders
    )
    rows = jnp.pad(pressure.reshape(2 * cycles, lon_local), ((0, 0), (0, lon_pad - lon_local)))
    starts = (
        lon_local * jnp.arange(no, dtype=jnp.int32)[:, None]
        + LANES * jnp.arange(tiles, dtype=jnp.int32)[None, :]
    )
    cos_q, sin_q = cos_sin(my_orders[None, :, None] * starts[:, None, :], period)
    cos_r, sin_r = cos_sin(my_orders[:, None] * jnp.arange(LANES, dtype=jnp.int32)[None, :], period)
    matches = cycle_list[:, None] == jnp.arange(half_total, dtype=jnp.int32)[None, :]
    weight = jnp.sum(jnp.where(matches, quad_weight[None, :], 0.0), axis=1) * (
        1.0 / math.sqrt(half_total)
    )
    eye = jnp.tile(jnp.eye(cycles, dtype=F32), (1, go))
    spread = weight[:, None] * eye * (1.0 / math.sqrt(period))
    fold = jnp.stack(
        [
            jnp.concatenate([spread, spread], 0),
            -jnp.concatenate([spread, spread], 0),
            jnp.concatenate([spread, -spread], 0),
            -jnp.concatenate([spread, -spread], 0),
        ]
    )
    zero = jnp.zeros_like(eye)
    sel = jnp.stack([jnp.concatenate([eye, zero], 0), jnp.concatenate([zero, eye], 0)]).astype(BF16)
    love = (DENSITY_RATIO * (1.0 + love_number))[None, :]
    love = lax.dynamic_slice_in_dim(love, lax.axis_index("lat") * share, share, 1)

    vmem = pl.BlockSpec(memory_space=pltpu.VMEM)
    spectrum, field = pl.pallas_call(
        functools.partial(kernel, n, no, cycles, lon_local),
        out_shape=(
            jax.ShapeDtypeStruct((2, local_orders, share), F32),
            jax.ShapeDtypeStruct((2 * cycles, lon_local), F32),
        ),
        in_specs=[vmem, pl.BlockSpec(memory_space=pl.ANY)] + [vmem] * 8,
        out_specs=(vmem, vmem),
        scratch_shapes=[
            pltpu.VMEM((local_orders * cycles, degrees), BF16),
            pltpu.VMEM((no, 2, local_orders, lon_pad), BF16),
            pltpu.VMEM((no - 1, 2 * cycles, lon_pad), BF16),
            pltpu.VMEM((4, local_orders, rows_g), F32),
            pltpu.VMEM((GROUPS, n, 2 * go, share), BF16),
            pltpu.VMEM((GROUPS, n, 2 * go, share), BF16),
            pltpu.VMEM((GROUPS, n, 2 * go, share), BF16),
            pltpu.VMEM((4, local_orders, rows_g), F32),
            pltpu.VMEM((no - 1, 2 * cycles, lon_pad), F32),
            pltpu.VMEM((no - 1, 2 * cycles, lon_pad), F32),
            pltpu.SemaphoreType.DMA((GROUPS,)),
            pltpu.SemaphoreType.DMA((2, no - 1)),
            pltpu.SemaphoreType.DMA((2, GROUPS, bits)),
            pltpu.SemaphoreType.DMA((2, GROUPS, bits)),
            pltpu.SemaphoreType.DMA((2, no - 1)),
        ],
        compiler_params=pltpu.CompilerParams(
            collective_id=0, has_side_effects=True, vmem_limit_bytes=56 * 1024 * 1024
        ),
    )(
        rows, tables.reshape(local_orders * cycles, degrees), cos_q, sin_q, cos_r, sin_r,
        my_orders[:, None], fold, sel, love,
    )
    return spectrum, field.reshape(2, cycles, lon_local)


def solution(mesh):
    placed = (P(None, "lat", "ord"), P("ord", "lat", None), P(), P(), P(), P("lat"))
    return jax.shard_map(
        functools.partial(per_device, mesh.shape["lat"], mesh.shape["ord"]),
        mesh=mesh,
        in_specs=placed,
        out_specs=(P(None, "ord", "lat"), P(None, "lat", "ord")),
        check_vma=False,
    )
```

```python
import functools
import math

import jax
import jax.numpy as jnp
from jax import lax
from jax.experimental import pallas as pl
from jax.experimental.pallas import tpu as pltpu
from jax.sharding import PartitionSpec as P

DENSITY_RATIO = 3.0 * 1025.0 / 5517.0
LANES = 128
GROUPS = 8
SETS = 2
STAGGER = 4
MESH = pl.DeviceIdType.MESH
NT = (((1,), (1,)), ((), ()))
F32 = jnp.float32
BF16 = jnp.bfloat16


def bit_orders(bits):
    base = list(range(bits))
    if bits < 3:
        return [base] * GROUPS
    a = base
    b = [1, 0] + base[2:]
    c = [2, 0, 1] + base[3:]
    d = [2, 1, 0] + base[3:]
    return [a, b, c, a, b, d, a, b]


def permuted(index, order):
    bits = len(order)
    return sum(((index // 2**b) % 2) * 2 ** (bits - 1 - at) for at, b in enumerate(order))


def cos_sin(count, period):
    turns = count - jnp.floor(count * (1.0 / period)) * period
    quarter = jnp.floor(turns * (4.0 / period) + 0.5)
    x = (turns - quarter * (period / 4.0)) * (2.0 * math.pi / period)
    y = x * x
    s = x * (1.0 + y * (-1.0 / 6 + y * (1.0 / 120 + y * (-1.0 / 5040 + y * (1.0 / 362880)))))
    c = 1.0 + y * (-0.5 + y * (1.0 / 24 + y * (-1.0 / 720 + y * (1.0 / 40320))))
    which = quarter.astype(jnp.int32) & 3
    swap = (which & 1) == 1
    cos = jnp.where(swap, s, c)
    sin = jnp.where(swap, c, s)
    return (
        jnp.where((which == 1) | (which == 2), -cos, cos),
        jnp.where(which >= 2, -sin, sin),
    )


def kernel(
    n, no,
    press_ref, tables_ref, quad_ref, love_ref, order_ref, cycle_ref,
    spec_ref, field_ref,
    tab, wave, gathered, padded, cos_q, sin_q, cos_r, sin_r, orders_ref, lhs, part, landed, scaled,
    picked, own_piece, out_piece, in_piece,
    tab_sem, press_sem, rs_sem, ag_sem, field_sem,
):
    bits = n.bit_length() - 1
    me = lax.axis_index("lat")
    core = lax.axis_index("ord")
    cycles = press_ref.shape[1]
    lon_local = press_ref.shape[2]
    local_orders = orders_ref.shape[0]
    degrees = tables_ref.shape[1]
    share = degrees // n
    go = local_orders // GROUPS
    set_orders = local_orders // SETS
    rows_g = go * cycles
    blocks = max(1, min(n, 1024 // share))
    width = blocks * share
    orders_of = bit_orders(bits)
    lon_pad = wave.shape[3]
    period = lon_local * no

    barrier = pltpu.get_barrier_semaphore()
    partners = []
    for b in range(bits):
        mine = (me // 2**b) % 2
        partners.append(me + (1 - 2 * mine) * 2**b)
    peers = [lax.rem(core + i, no) for i in range(1, no)]
    for partner in partners:
        pl.semaphore_signal(barrier, inc=1, device_id=(partner, core), device_id_type=MESH)
    for peer in peers:
        pl.semaphore_signal(barrier, inc=1, device_id=(me, peer), device_id_type=MESH)

    tab_copies = []
    for g in range(GROUPS):
        rows = pl.ds(g * rows_g, rows_g)
        copy = pltpu.make_async_copy(tables_ref.at[rows], tab.at[rows], tab_sem.at[g])
        copy.start()
        tab_copies.append(copy)

    pl.semaphore_wait(barrier, bits + no - 1)
    press_copies = []
    for i, peer in enumerate(peers):
        copy = pltpu.make_async_remote_copy(
            src_ref=press_ref,
            dst_ref=gathered.at[i],
            send_sem=press_sem.at[0, i],
            recv_sem=press_sem.at[1, i],
            device_id=(me, peer),
            device_id_type=MESH,
        )
        copy.start()
        press_copies.append(copy)

    shape = (local_orders, order_ref.shape[1])
    slot = core * local_orders + lax.broadcasted_iota(jnp.int32, shape, 0)
    hit = slot == lax.broadcasted_iota(jnp.int32, shape, 1)
    order_col = jnp.sum(jnp.where(hit, order_ref[...].astype(F32), 0.0), axis=1, keepdims=True)
    orders_ref[...] = order_col.astype(jnp.int32)
    lane = lax.broadcasted_iota(jnp.int32, (local_orders, LANES), 1)
    cos_r[...], sin_r[...] = cos_sin(order_col * lane.astype(F32), period)
    for p in range(no):
        start = (p * lon_local + LANES * lane).astype(F32)
        cos_q[p], sin_q[p] = cos_sin(order_col * start, period)

    fold_shape = (2 * cycles, rows_g)
    fold_row = lax.broadcasted_iota(jnp.int32, fold_shape, 0)
    fold_col = lax.broadcasted_iota(jnp.int32, fold_shape, 1) % cycles
    spread = jnp.zeros(fold_shape, F32)
    quad_lane = lax.broadcasted_iota(jnp.int32, quad_ref.shape, 1)
    for j in range(cycles):
        weight = jnp.sum(
            jnp.where(quad_lane == cycle_ref[j], quad_ref[...], 0.0), axis=1, keepdims=True
        ) * (1.0 / math.sqrt(quad_ref.shape[1]))
        spread = jnp.where((fold_row % cycles == j) & (fold_col == j), weight, spread)
    spread = spread * (1.0 / math.sqrt(period))
    fold_sum = jnp.concatenate([spread, jnp.where(fold_row < cycles, spread, -spread)], 1)

    def selector(half):
        return jnp.where(fold_row == fold_col + half * cycles, 1.0, 0.0).astype(BF16)

    col = lax.broadcasted_iota(jnp.int32, (set_orders, rows_g), 1) // cycles
    row = lax.broadcasted_iota(jnp.int32, (set_orders, rows_g), 0) % go
    diagonal = row == col

    def pad_rows(at, piece):
        padded[at] = jnp.zeros(padded.shape[1:], BF16)
        both = jnp.concatenate([piece[0].astype(F32), piece[1].astype(F32)], 0)
        padded[at, :, :lon_local] = both.astype(BF16)

    def prepare(s):
        mine = slice(s * set_orders, (s + 1) * set_orders)

        def make_wave(p, carry):
            for q in range(lon_pad // LANES):
                cq = cos_q[p, mine, q : q + 1]
                sq = sin_q[p, mine, q : q + 1]
                cols = slice(q * LANES, (q + 1) * LANES)
                wave[p, s, :set_orders, cols] = (cq * cos_r[mine] - sq * sin_r[mine]).astype(BF16)
                wave[p, s, set_orders:, cols] = (sq * cos_r[mine] + cq * sin_r[mine]).astype(BF16)
            return carry

        lax.fori_loop(0, no, make_wave, 0)
        if s == 0:
            pad_rows(0, press_ref)
            for i, copy in enumerate(press_copies):
                copy.wait()
                pad_rows(i + 1, gathered.at[i])
        sums = jnp.zeros((2 * set_orders, 2 * cycles), F32)
        for i in range(no):
            origin = lax.rem(core + no - i, no)
            sums = sums + lax.dot_general(
                wave[origin, s], padded[i], NT, preferred_element_type=F32
            )
        value = jnp.dot(
            sums, fold_sum, precision=lax.Precision.HIGHEST, preferred_element_type=F32
        )
        for f in range(2):
            half = value[:, f * rows_g : (f + 1) * rows_g]
            lhs[2 * f, mine] = jnp.where(diagonal, half[:set_orders], 0.0)
            lhs[2 * f + 1, mine] = jnp.where(diagonal, -half[set_orders:], 0.0)

    def parity(g, first):
        degree = first + lax.broadcasted_iota(jnp.int32, (go, width), 1)
        order = orders_ref[g * go : (g + 1) * go, :]
        return (degree + order) & 1 == 0, degree >= order

    def region(g, k):
        base = 0
        for at in range(k):
            base = base + ((me // 2 ** orders_of[g][at]) % 2) * (n >> (at + 1))
        return base

    def analyse(g):
        tab_copies[g].wait()
        left = jnp.concatenate([lhs[c, g * go : (g + 1) * go, :] for c in range(4)], 0).astype(BF16)

        def chunk(i, carry):
            first = pl.multiple_of(i * width, width)
            product = jnp.dot(
                left, tab[g * rows_g : (g + 1) * rows_g, pl.ds(first, width)], preferred_element_type=F32
            )
            even, present = parity(g, first)
            real = jnp.where(present, jnp.where(even, product[:go], product[2 * go : 3 * go]), 0.0)
            imag = jnp.where(present, jnp.where(even, product[go : 2 * go], product[3 * go :]), 0.0)
            value = jnp.concatenate([real, imag], 0).astype(BF16)
            for j in range(blocks):
                to = permuted(i * blocks + j, orders_of[g])
                part[g, to] = value[:, j * share : (j + 1) * share]
            return carry

        lax.fori_loop(0, degrees // width, chunk, 0)

    reduce_copies = {}
    gather_copies = {}

    def send_reduce(g, k):
        h = n >> (k + 1)
        b = orders_of[g][k]
        mine = (me // 2**b) % 2
        copy = pltpu.make_async_remote_copy(
            src_ref=part.at[g, pl.ds(region(g, k) + (1 - mine) * h, h)],
            dst_ref=landed.at[g, pl.ds(n - (n >> k), h)],
            send_sem=rs_sem.at[0, g, k],
            recv_sem=rs_sem.at[1, g, k],
            device_id=(partners[b], core),
            device_id_type=MESH,
        )
        copy.start()
        reduce_copies[g, k] = copy

    def take_reduce(g, k):
        h = n >> (k + 1)
        reduce_copies[g, k].wait_recv()
        keep = region(g, k + 1)
        off = n - (n >> k)
        if k < bits - 1:

            def add(i, carry):
                part[g, keep + i] = (
                    part[g, keep + i].astype(F32) + landed[g, off + i].astype(F32)
                ).astype(BF16)
                return carry

            lax.fori_loop(0, h, add, 0, unroll=min(h, 4))
            send_reduce(g, k + 1)
            return
        total = part[g, keep].astype(F32) + landed[g, off].astype(F32)
        spec_ref[0, g * go : (g + 1) * go, :] = total[:go]
        spec_ref[1, g * go : (g + 1) * go, :] = total[go:]
        scaled[g, keep] = (DENSITY_RATIO * (1.0 + love_ref[pl.ds(me, 1), :]) * total).astype(BF16)
        send_gather(g, bits - 1)

    def send_gather(g, k):
        h = n >> (k + 1)
        b = orders_of[g][k]
        mine = pl.ds(region(g, k + 1), h)
        copy = pltpu.make_async_remote_copy(
            src_ref=scaled.at[g, mine],
            dst_ref=scaled.at[g, mine],
            send_sem=ag_sem.at[0, g, k],
            recv_sem=ag_sem.at[1, g, k],
            device_id=(partners[b], core),
            device_id_type=MESH,
        )
        copy.start()
        gather_copies[g, k] = copy

    def take_gather(g, k):
        gather_copies[g, k].wait_recv()
        if k > 0:
            send_gather(g, k - 1)

    def synthesise(g):
        def chunk(i, total):
            first = pl.multiple_of(i * width, width)
            even, _ = parity(g, first)
            pieces = [scaled[g, permuted(i * blocks + j, orders_of[g])] for j in range(blocks)]
            both = jnp.concatenate(pieces, 1).astype(F32)
            real, imag = both[:go], both[go:]
            stacked = jnp.concatenate(
                [real, imag, jnp.where(even, real, -real), jnp.where(even, imag, -imag)], 0
            ).astype(BF16)
            return total + lax.dot_general(
                stacked, tab[g * rows_g : (g + 1) * rows_g, pl.ds(first, width)], NT,
                preferred_element_type=F32,
            )

        total = lax.fori_loop(0, degrees // width, chunk, jnp.zeros((4 * go, rows_g), F32))
        total = total * (1.0 / math.sqrt(degrees))
        keep = diagonal[:go]
        for c in range(4):
            picked[c, g * go : (g + 1) * go, :] = jnp.where(keep, total[c * go : (c + 1) * go], 0.0)

    def synthesise_set(s):
        mine = slice(s * set_orders, (s + 1) * set_orders)
        signal = []
        for t in range(2):
            north, south = [
                lax.dot_general(
                    selector(half), picked[2 * half + t, mine].astype(BF16), NT,
                    preferred_element_type=F32,
                )
                for half in range(2)
            ]
            signal.append(north + south)
        both = jnp.concatenate([signal[0], -signal[1]], 1).astype(BF16)
        for i, peer in enumerate(peers + [core]):
            total = jnp.dot(both, wave[peer, s], preferred_element_type=F32)
            ref = own_piece if i == no - 1 else out_piece.at[i]
            ref[...] = total if s == 0 else ref[...] + total
            if s == SETS - 1 and i < no - 1:
                copy = pltpu.make_async_remote_copy(
                    src_ref=out_piece.at[i],
                    dst_ref=in_piece.at[i],
                    send_sem=field_sem.at[0, i],
                    recv_sem=field_sem.at[1, i],
                    device_id=(me, peer),
                    device_id_type=MESH,
                )
                copy.start()
                field_copies.append(copy)

    field_copies = []
    steps = []
    per_set = GROUPS // SETS
    for s in range(SETS):
        steps.append((s * per_set - 0.5, s, lambda s=s: prepare(s)))
    for g in range(GROUPS):
        steps.append((g, g, lambda g=g: (analyse(g), send_reduce(g, 0))))
        for k in range(bits):
            steps.append((g + STAGGER * (k + 1), g, lambda g=g, k=k: take_reduce(g, k)))
        for i, k in enumerate(reversed(range(bits))):
            steps.append((g + STAGGER * (bits + i + 1), g, lambda g=g, k=k: take_gather(g, k)))
        steps.append((g + STAGGER * 2 * bits + 0.5, g, lambda g=g: synthesise(g)))
    for s in range(SETS):
        last = (s + 1) * per_set - 1
        steps.append((last + STAGGER * 2 * bits + 0.75, s, lambda s=s: synthesise_set(s)))
    for _, _, step in sorted(steps, key=lambda s: (s[0], s[1])):
        step()

    total = own_piece[...]
    for i, copy in enumerate(field_copies):
        copy.wait_recv()
        total = total + in_piece[i]
    total = total[:, :lon_local] * (1.0 / math.sqrt(local_orders * no))
    field_ref[0] = total[:cycles]
    field_ref[1] = total[cycles:]
    for copy in list(reduce_copies.values()) + list(gather_copies.values()) + field_copies:
        copy.wait_send()


def per_device(n, no, pressure, tables, quad_weight, love_number, order_list, cycle_list):
    _, cycles, lon_local = pressure.shape
    local_orders, _, degrees = tables.shape
    bits = n.bit_length() - 1
    share = degrees // n
    go = local_orders // GROUPS
    rows_g = go * cycles
    lon_pad = -(-lon_local // LANES) * LANES
    vmem = pl.BlockSpec(memory_space=pltpu.VMEM)
    table = pltpu.VMEM((local_orders, LANES), F32)
    tables_q = pltpu.VMEM((no, local_orders, LANES), F32)
    blocks = pltpu.VMEM((GROUPS, n, 2 * go, share), BF16)
    pieces = pltpu.VMEM((no - 1, 2 * cycles, lon_pad), F32)
    return pl.pallas_call(
        functools.partial(kernel, n, no),
        out_shape=(
            jax.ShapeDtypeStruct((2, local_orders, share), F32),
            jax.ShapeDtypeStruct((2, cycles, lon_local), F32),
        ),
        in_specs=[
            vmem, pl.BlockSpec(memory_space=pl.ANY), vmem, vmem, vmem,
            pl.BlockSpec(memory_space=pltpu.SMEM),
        ],
        out_specs=(vmem, vmem),
        scratch_shapes=[
            pltpu.VMEM((local_orders * cycles, degrees), BF16),
            pltpu.VMEM((no, SETS, 2 * local_orders // SETS, lon_pad), BF16),
            pltpu.VMEM((no - 1, 2, cycles, lon_local), BF16),
            pltpu.VMEM((no, 2 * cycles, lon_pad), BF16),
            tables_q, tables_q, table, table,
            pltpu.VMEM((local_orders, 1), jnp.int32),
            pltpu.VMEM((4, local_orders, rows_g), F32),
            blocks, blocks, blocks,
            pltpu.VMEM((4, local_orders, rows_g), F32),
            pltpu.VMEM((2 * cycles, lon_pad), F32),
            pieces, pieces,
            pltpu.SemaphoreType.DMA((GROUPS,)),
            pltpu.SemaphoreType.DMA((2, no - 1)),
            pltpu.SemaphoreType.DMA((2, GROUPS, bits)),
            pltpu.SemaphoreType.DMA((2, GROUPS, bits)),
            pltpu.SemaphoreType.DMA((2, no - 1)),
        ],
        compiler_params=pltpu.CompilerParams(
            collective_id=0, has_side_effects=True, vmem_limit_bytes=56 * 1024 * 1024
        ),
    )(
        pressure, tables.reshape(local_orders * cycles, degrees), quad_weight[None, :],
        love_number.reshape(n, share), order_list[None, :], cycle_list,
    )


def solution(mesh):
    placed = (P(None, "lat", "ord"), P("ord", "lat", None), P(), P(), P(), P("lat"))
    return jax.shard_map(
        functools.partial(per_device, mesh.shape["lat"], mesh.shape["ord"]),
        mesh=mesh,
        in_specs=placed,
        out_specs=(P(None, "ord", "lat"), P(None, "lat", "ord")),
        check_vma=False,
    )
```

```python
import functools
import math

import jax
import jax.numpy as jnp
from jax import lax
from jax.experimental import pallas as pl
from jax.experimental.pallas import tpu as pltpu
from jax.sharding import PartitionSpec as P

DENSITY_RATIO = 3.0 * 1025.0 / 5517.0
LANES = 128
GROUPS = 8
SETS = 4
STAGGER = 4
MESH = pl.DeviceIdType.MESH
NT = (((1,), (1,)), ((), ()))
F32 = jnp.float32
BF16 = jnp.bfloat16


def bit_orders(bits):
    base = list(range(bits))
    if bits < 3:
        return [base] * GROUPS
    a = base
    b = [1, 0] + base[2:]
    c = [2, 0, 1] + base[3:]
    d = [2, 1, 0] + base[3:]
    e = [0, 2, 1] + base[3:]
    f = [1, 2, 0] + base[3:]
    return [a, b, c, e, f, d, a, b]


def permuted(index, order):
    bits = len(order)
    return sum(((index // 2**b) % 2) * 2 ** (bits - 1 - at) for at, b in enumerate(order))


def cos_sin(count, period):
    turns = count - jnp.floor(count * (1.0 / period)) * period
    quarter = jnp.floor(turns * (4.0 / period) + 0.5)
    x = (turns - quarter * (period / 4.0)) * (2.0 * math.pi / period)
    y = x * x
    s = x * (1.0 + y * (-1.0 / 6 + y * (1.0 / 120 + y * (-1.0 / 5040 + y * (1.0 / 362880)))))
    c = 1.0 + y * (-0.5 + y * (1.0 / 24 + y * (-1.0 / 720 + y * (1.0 / 40320))))
    which = quarter.astype(jnp.int32) & 3
    swap = (which & 1) == 1
    cos = jnp.where(swap, s, c)
    sin = jnp.where(swap, c, s)
    return (
        jnp.where((which == 1) | (which == 2), -cos, cos),
        jnp.where(which >= 2, -sin, sin),
    )


def kernel(
    n, no,
    press_ref, tables_ref, quad_ref, love_ref, order_ref, cycle_ref,
    spec_ref, total_ref,
    tab, wave, gathered, padded, cos_q, sin_q, cos_r, sin_r, orders_ref, lhs, part, landed, scaled,
    picked, own_piece, out_piece, in_piece,
    tab_sem, press_sem, rs_sem, ag_sem, field_sem,
):
    bits = n.bit_length() - 1
    me = lax.axis_index("lat")
    core = lax.axis_index("ord")
    cycles = press_ref.shape[1]
    lon_local = press_ref.shape[2]
    local_orders = orders_ref.shape[0]
    degrees = tables_ref.shape[1]
    share = degrees // n
    go = local_orders // GROUPS
    set_orders = local_orders // SETS
    rows_g = go * cycles
    blocks = max(1, min(n, 1024 // share))
    width = blocks * share
    orders_of = bit_orders(bits)
    lon_pad = wave.shape[3]
    period = lon_local * no

    barrier = pltpu.get_barrier_semaphore()
    partners = []
    for b in range(bits):
        mine = (me // 2**b) % 2
        partners.append(me + (1 - 2 * mine) * 2**b)
    peers = [lax.rem(core + i, no) for i in range(1, no)]
    for partner in partners:
        pl.semaphore_signal(barrier, inc=1, device_id=(partner, core), device_id_type=MESH)
    for peer in peers:
        pl.semaphore_signal(barrier, inc=1, device_id=(me, peer), device_id_type=MESH)

    tab_copies = []
    for g in range(GROUPS):
        rows = pl.ds(g * rows_g, rows_g)
        copy = pltpu.make_async_copy(tables_ref.at[rows], tab.at[rows], tab_sem.at[g])
        copy.start()
        tab_copies.append(copy)

    pl.semaphore_wait(barrier, bits + no - 1)
    press_copies = []
    for i, peer in enumerate(peers):
        copy = pltpu.make_async_remote_copy(
            src_ref=press_ref,
            dst_ref=gathered.at[i],
            send_sem=press_sem.at[0, i],
            recv_sem=press_sem.at[1, i],
            device_id=(me, peer),
            device_id_type=MESH,
        )
        copy.start()
        press_copies.append(copy)

    shape = (local_orders, order_ref.shape[1])
    slot = core * local_orders + lax.broadcasted_iota(jnp.int32, shape, 0)
    hit = slot == lax.broadcasted_iota(jnp.int32, shape, 1)
    order_col = jnp.sum(jnp.where(hit, order_ref[...].astype(F32), 0.0), axis=1, keepdims=True)
    orders_ref[...] = order_col.astype(jnp.int32)
    lane = lax.broadcasted_iota(jnp.int32, (local_orders, LANES), 1)
    cos_r[...], sin_r[...] = cos_sin(order_col * lane.astype(F32), period)
    for p in range(no):
        start = (p * lon_local + LANES * lane).astype(F32)
        cos_q[p], sin_q[p] = cos_sin(order_col * start, period)

    fold_shape = (2 * cycles, rows_g)
    fold_row = lax.broadcasted_iota(jnp.int32, fold_shape, 0)
    fold_col = lax.broadcasted_iota(jnp.int32, fold_shape, 1) % cycles
    spread = jnp.zeros(fold_shape, F32)
    quad_lane = lax.broadcasted_iota(jnp.int32, quad_ref.shape, 1)
    for j in range(cycles):
        weight = jnp.sum(
            jnp.where(quad_lane == cycle_ref[j], quad_ref[...], 0.0), axis=1, keepdims=True
        ) * (1.0 / math.sqrt(quad_ref.shape[1]))
        spread = jnp.where((fold_row % cycles == j) & (fold_col == j), weight, spread)
    spread = spread * (1.0 / math.sqrt(period))
    fold_sum = jnp.concatenate([spread, jnp.where(fold_row < cycles, spread, -spread)], 1)

    def selector(half):
        return jnp.where(fold_row == fold_col + half * cycles, 1.0, 0.0).astype(BF16)

    col = lax.broadcasted_iota(jnp.int32, (set_orders, rows_g), 1) // cycles
    row = lax.broadcasted_iota(jnp.int32, (set_orders, rows_g), 0) % go
    diagonal = row == col

    def pad_rows(at, piece):
        padded[at] = jnp.zeros(padded.shape[1:], BF16)
        both = jnp.concatenate([piece[0].astype(F32), piece[1].astype(F32)], 0)
        padded[at, :, :lon_local] = both.astype(BF16)

    def prepare(s):
        mine = slice(s * set_orders, (s + 1) * set_orders)

        def make_wave(p, carry):
            for q in range(lon_pad // LANES):
                cq = cos_q[p, mine, q : q + 1]
                sq = sin_q[p, mine, q : q + 1]
                cols = slice(q * LANES, (q + 1) * LANES)
                wave[p, s, :set_orders, cols] = (cq * cos_r[mine] - sq * sin_r[mine]).astype(BF16)
                wave[p, s, set_orders:, cols] = (sq * cos_r[mine] + cq * sin_r[mine]).astype(BF16)
            return carry

        lax.fori_loop(0, no, make_wave, 0)
        if s == 0:
            pad_rows(0, press_ref)
            for i, copy in enumerate(press_copies):
                copy.wait()
                pad_rows(i + 1, gathered.at[i])
        sums = jnp.zeros((2 * set_orders, 2 * cycles), F32)
        for i in range(no):
            origin = lax.rem(core + no - i, no)
            sums = sums + lax.dot_general(
                wave[origin, s], padded[i], NT, preferred_element_type=F32
            )
        value = jnp.dot(
            sums, fold_sum, precision=lax.Precision.HIGHEST, preferred_element_type=F32
        )
        for f in range(2):
            half = value[:, f * rows_g : (f + 1) * rows_g]
            lhs[2 * f, mine] = jnp.where(diagonal, half[:set_orders], 0.0)
            lhs[2 * f + 1, mine] = jnp.where(diagonal, -half[set_orders:], 0.0)

    def parity(g, first):
        degree = first + lax.broadcasted_iota(jnp.int32, (go, width), 1)
        order = orders_ref[g * go : (g + 1) * go, :]
        return (degree + order) & 1 == 0, degree >= order

    def region(g, k):
        base = 0
        for at in range(k):
            base = base + ((me // 2 ** orders_of[g][at]) % 2) * (n >> (at + 1))
        return base

    def analyse(g):
        tab_copies[g].wait()
        left = jnp.concatenate([lhs[c, g * go : (g + 1) * go, :] for c in range(4)], 0).astype(BF16)

        def chunk(i, carry):
            first = pl.multiple_of(i * width, width)
            product = jnp.dot(
                left, tab[g * rows_g : (g + 1) * rows_g, pl.ds(first, width)], preferred_element_type=F32
            )
            even, present = parity(g, first)
            real = jnp.where(present, jnp.where(even, product[:go], product[2 * go : 3 * go]), 0.0)
            imag = jnp.where(present, jnp.where(even, product[go : 2 * go], product[3 * go :]), 0.0)
            value = jnp.concatenate([real, imag], 0).astype(BF16)
            for j in range(blocks):
                to = permuted(i * blocks + j, orders_of[g])
                part[g, to] = value[:, j * share : (j + 1) * share]
            return carry

        lax.fori_loop(0, degrees // width, chunk, 0)

    reduce_copies = {}
    gather_copies = {}

    def send_reduce(g, k):
        h = n >> (k + 1)
        b = orders_of[g][k]
        mine = (me // 2**b) % 2
        copy = pltpu.make_async_remote_copy(
            src_ref=part.at[g, pl.ds(region(g, k) + (1 - mine) * h, h)],
            dst_ref=landed.at[g, pl.ds(n - (n >> k), h)],
            send_sem=rs_sem.at[0, g, k],
            recv_sem=rs_sem.at[1, g, k],
            device_id=(partners[b], core),
            device_id_type=MESH,
        )
        copy.start()
        reduce_copies[g, k] = copy

    def take_reduce(g, k):
        h = n >> (k + 1)
        reduce_copies[g, k].wait_recv()
        keep = region(g, k + 1)
        off = n - (n >> k)
        if k < bits - 1:

            def add(i, carry):
                part[g, keep + i] = (
                    part[g, keep + i].astype(F32) + landed[g, off + i].astype(F32)
                ).astype(BF16)
                return carry

            lax.fori_loop(0, h, add, 0, unroll=min(h, 4))
            send_reduce(g, k + 1)
            return
        total = part[g, keep].astype(F32) + landed[g, off].astype(F32)
        spec_ref[0, g * go : (g + 1) * go, :] = total[:go]
        spec_ref[1, g * go : (g + 1) * go, :] = total[go:]
        scaled[g, keep] = (DENSITY_RATIO * (1.0 + love_ref[pl.ds(me, 1), :]) * total).astype(BF16)
        send_gather(g, bits - 1)

    def send_gather(g, k):
        h = n >> (k + 1)
        b = orders_of[g][k]
        mine = pl.ds(region(g, k + 1), h)
        copy = pltpu.make_async_remote_copy(
            src_ref=scaled.at[g, mine],
            dst_ref=scaled.at[g, mine],
            send_sem=ag_sem.at[0, g, k],
            recv_sem=ag_sem.at[1, g, k],
            device_id=(partners[b], core),
            device_id_type=MESH,
        )
        copy.start()
        gather_copies[g, k] = copy

    def take_gather(g, k):
        gather_copies[g, k].wait_recv()
        if k > 0:
            send_gather(g, k - 1)

    def synthesise(g):
        def chunk(i, total):
            first = pl.multiple_of(i * width, width)
            even, _ = parity(g, first)
            pieces = [scaled[g, permuted(i * blocks + j, orders_of[g])] for j in range(blocks)]
            both = jnp.concatenate(pieces, 1).astype(F32)
            real, imag = both[:go], both[go:]
            stacked = jnp.concatenate(
                [real, imag, jnp.where(even, real, -real), jnp.where(even, imag, -imag)], 0
            ).astype(BF16)
            return total + lax.dot_general(
                stacked, tab[g * rows_g : (g + 1) * rows_g, pl.ds(first, width)], NT,
                preferred_element_type=F32,
            )

        total = lax.fori_loop(0, degrees // width, chunk, jnp.zeros((4 * go, rows_g), F32))
        total = total * (1.0 / math.sqrt(degrees))
        keep = diagonal[:go]
        for c in range(4):
            picked[c, g * go : (g + 1) * go, :] = jnp.where(keep, total[c * go : (c + 1) * go], 0.0)

    def synthesise_set(s):
        mine = slice(s * set_orders, (s + 1) * set_orders)
        signal = []
        for t in range(2):
            north, south = [
                lax.dot_general(
                    selector(half), picked[2 * half + t, mine].astype(BF16), NT,
                    preferred_element_type=F32,
                )
                for half in range(2)
            ]
            signal.append(north + south)
        both = jnp.concatenate([signal[0], -signal[1]], 1).astype(BF16)
        for i, peer in enumerate(peers + [core]):
            total = jnp.dot(both, wave[peer, s], preferred_element_type=F32)
            ref = own_piece if i == no - 1 else out_piece.at[i]
            ref[...] = total if s == 0 else ref[...] + total
            if s == SETS - 1 and i < no - 1:
                copy = pltpu.make_async_remote_copy(
                    src_ref=out_piece.at[i],
                    dst_ref=in_piece.at[i],
                    send_sem=field_sem.at[0, i],
                    recv_sem=field_sem.at[1, i],
                    device_id=(me, peer),
                    device_id_type=MESH,
                )
                copy.start()
                field_copies.append(copy)

    field_copies = []
    steps = []
    per_set = GROUPS // SETS
    for s in range(SETS):
        steps.append((s * per_set - 0.5, s, lambda s=s: prepare(s)))
    for g in range(GROUPS):
        steps.append((g, g, lambda g=g: (analyse(g), send_reduce(g, 0))))
        for k in range(bits):
            steps.append((g + STAGGER * (k + 1), g, lambda g=g, k=k: take_reduce(g, k)))
        for i, k in enumerate(reversed(range(bits))):
            steps.append((g + STAGGER * (bits + i + 1), g, lambda g=g, k=k: take_gather(g, k)))
        steps.append((g + STAGGER * 2 * bits + 0.5, g, lambda g=g: synthesise(g)))
    for s in range(SETS):
        last = (s + 1) * per_set - 1
        steps.append((last + STAGGER * 2 * bits + 0.75, s, lambda s=s: synthesise_set(s)))
    for _, _, step in sorted(steps, key=lambda s: (s[0], s[1])):
        step()

    for copy in field_copies:
        copy.wait_recv()
    total_ref[...] = own_piece[...]
    for i in range(no - 1):
        total_ref[...] += in_piece[i]
    for copy in list(reduce_copies.values()) + list(gather_copies.values()) + field_copies:
        copy.wait_send()


def finish(scale, half_spec, total_ref, spec_ref, field_ref):
    cycles, lon_local = field_ref.shape[1:]
    spec_ref[...] = half_spec[...]
    for h in range(2):
        field_ref[h] = total_ref[h * cycles : (h + 1) * cycles, :lon_local] * scale


def per_device(n, no, pressure, tables, quad_weight, love_number, order_list, cycle_list):
    _, cycles, lon_local = pressure.shape
    local_orders, _, degrees = tables.shape
    bits = n.bit_length() - 1
    share = degrees // n
    go = local_orders // GROUPS
    rows_g = go * cycles
    lon_pad = -(-lon_local // LANES) * LANES
    vmem = pl.BlockSpec(memory_space=pltpu.VMEM)
    table = pltpu.VMEM((local_orders, LANES), F32)
    tables_q = pltpu.VMEM((no, local_orders, LANES), F32)
    blocks = pltpu.VMEM((GROUPS, n, 2 * go, share), BF16)
    pieces = pltpu.VMEM((no - 1, 2 * cycles, lon_pad), F32)
    spectrum, total = pl.pallas_call(
        functools.partial(kernel, n, no),
        out_shape=(
            jax.ShapeDtypeStruct((2, local_orders, share), F32),
            jax.ShapeDtypeStruct((2 * cycles, lon_pad), F32),
        ),
        in_specs=[
            vmem, pl.BlockSpec(memory_space=pl.ANY), vmem, vmem, vmem,
            pl.BlockSpec(memory_space=pltpu.SMEM),
        ],
        out_specs=(vmem, vmem),
        scratch_shapes=[
            pltpu.VMEM((local_orders * cycles, degrees), BF16),
            pltpu.VMEM((no, SETS, 2 * local_orders // SETS, lon_pad), BF16),
            pltpu.VMEM((no - 1, 2, cycles, lon_local), BF16),
            pltpu.VMEM((no, 2 * cycles, lon_pad), BF16),
            tables_q, tables_q, table, table,
            pltpu.VMEM((local_orders, 1), jnp.int32),
            pltpu.VMEM((4, local_orders, rows_g), F32),
            blocks, blocks, blocks,
            pltpu.VMEM((4, local_orders, rows_g), F32),
            pltpu.VMEM((2 * cycles, lon_pad), F32),
            pieces, pieces,
            pltpu.SemaphoreType.DMA((GROUPS,)),
            pltpu.SemaphoreType.DMA((2, no - 1)),
            pltpu.SemaphoreType.DMA((2, GROUPS, bits)),
            pltpu.SemaphoreType.DMA((2, GROUPS, bits)),
            pltpu.SemaphoreType.DMA((2, no - 1)),
        ],
        compiler_params=pltpu.CompilerParams(
            collective_id=0, has_side_effects=True, vmem_limit_bytes=56 * 1024 * 1024
        ),
    )(
        pressure, tables.reshape(local_orders * cycles, degrees), quad_weight[None, :],
        love_number.reshape(n, share), order_list[None, :], cycle_list,
    )
    return pl.pallas_call(
        functools.partial(finish, 1.0 / math.sqrt(local_orders * no)),
        out_shape=(
            jax.ShapeDtypeStruct(spectrum.shape, F32),
            jax.ShapeDtypeStruct((2, cycles, lon_local), F32),
        ),
        in_specs=[vmem, vmem],
        out_specs=(vmem, vmem),
    )(spectrum, total)


def solution(mesh):
    placed = (P(None, "lat", "ord"), P("ord", "lat", None), P(), P(), P(), P("lat"))
    return jax.shard_map(
        functools.partial(per_device, mesh.shape["lat"], mesh.shape["ord"]),
        mesh=mesh,
        in_specs=placed,
        out_specs=(P(None, "ord", "lat"), P(None, "lat", "ord")),
        check_vma=False,
    )
```
